32 devices in a mesh: fsdp: 16 (over z, x, core), tp: 2 (over y).
Axes of the slice: x: 2, y: 2, z: 4, core: 2. Of those that a mesh axis runs over, the one named last changes fastest.
Arguments:
- hidden: bfloat16 [4096, 8192], P('fsdp'), may hold values from -6 to 6
- norm_gain: float32 [8192], replicated, may hold values from 0.6 to 6, as said below
- w_query: bfloat16 [8192, 4096], P('fsdp', 'tp'), may hold values from -0.09375 to 0.09375
- w_key: bfloat16 [8192, 512], P('fsdp'), may hold values from -0.09375 to 0.09375
- w_value: bfloat16 [8192, 512], P('fsdp'), may hold values from -0.0625 to 0.0625
- bias_query: bfloat16 [4096], P('tp'), may hold values from -3 to 3
- bias_key: bfloat16 [512], replicated, may hold values from -3 to 3
- bias_value: bfloat16 [512], replicated, may hold values from -3 to 3
- w_out: bfloat16 [4096, 8192], P('tp', 'fsdp'), may hold values from -0.09375 to 0.09375
- seq_lengths: int32 [4], replicated, may hold values from 1 to 3072, 4096 in all
Outputs:
- hidden_out: float32 [4096, 8192], P(('fsdp', 'tp'))
The draws below stay inside these ranges and needn't reach their ends.
Inputs may be any that keep to these rules, and one draw needn't show every extreme that they name: `seq_lengths`: 4 sequences packed in order; the lengths sum to 4096 and the longest has exactly 3072 tokens. `norm_gain`: positive gains.
All inputs are finite; a program needn't handle non-finite values.
Results may differ from the reference program's by a relative error of at most 0.014.
The reference program's roundings to bfloat16 on the way count: a program that leaves them out, or rounds other values in their place, can miss the bound.
Values may be sent and summed in bfloat16 or wider, within the bound.
A program may use at most 128 MiB of HBM per device.

```python
import math
import jax
import jax.numpy as jnp
import numpy as np
from jax import lax

D = 8192
HEAD = 128
QHEADS = 32
KVHEADS = 4
SEQS = 4
TOKENS = 4096
LONGEST = 3072


def draw_norm_gain(key, part):
    lower, upper = (math.log(0.6), math.log(2.0))
    return jnp.exp(jax.random.uniform(key, (D,), jnp.float32, lower, upper))


def levels(own_key, extent, shards, least, top_value):
    loudness = 1.0
    for axis_at, blocks in shards:
        steps = jax.random.uniform(jax.random.fold_in(jax.random.fold_in(own_key, 6), axis_at), (blocks,), jnp.float32, least / len(shards), top_value / len(shards))
        loudness = loudness * jnp.repeat(jnp.exp(steps), extent[axis_at] // blocks).reshape((-1,) + (1,) * (len(extent) - 1 - axis_at))
    return loudness


def length_profile(number_of, total, bound, slope):
    weights = [(1 << 20) // math.isqrt(standing ** slope) + 1 for standing in range(2, number_of + 1)]
    surplus, holding = total - bound - (number_of - 1), [1] * (number_of - 1)
    while surplus > 0:
        movable = [i for i in range(number_of - 1) if holding[i] < bound]
        whole, left = sum([weights[i] for i in movable]), surplus
        for i in movable:
            more = min(bound - holding[i], max(1, left * weights[i] // whole), surplus)
            holding[i] = holding[i] + more
            surplus = surplus - more
    return np.array([bound] + holding)


def uneven(key, count, total, reach, slope):
    if count == 2:
        one = jax.random.randint(key, (), max(1, total - reach), min(reach, total - 1) + 1)
        return jnp.stack([one, total - one])
    tallies = jnp.asarray(length_profile(count, total, reach, slope), jnp.int32)
    couples = (count - 1) // 2
    donor, taker = tallies[1:1 + 2 * couples:2], tallies[2:2 + 2 * couples:2]
    margin = jnp.minimum(donor - 1, reach - taker)
    moved = jax.random.randint(jax.random.fold_in(key, 1), (couples,), 0, 1 << 20) % (margin + 1)
    tallies = tallies.at[1:1 + 2 * couples:2].set(donor - moved).at[2:2 + 2 * couples:2].set(taker + moved)
    return tallies[jax.random.permutation(jax.random.fold_in(key, 2), count)]


def noise(key, shape, deviation, reach, shards=(), held_as=jnp.bfloat16):
    result = jax.random.normal(key, shape, jnp.float32) * deviation
    if len(shards) > 0:
        result = levels(key, shape, shards, -0.22, 0.18) * result
    return jnp.clip(result, min=-reach, max=reach).astype(held_as)


def setup_inputs(seed: int = 0) -> dict:
    key_list = jax.random.split(jax.random.key(seed), 11)
    return {
        "hidden": noise(key_list[0], (TOKENS, D), 1.0, 6.0, ((0, 16),)),
        "norm_gain": draw_norm_gain(jax.random.fold_in(key_list[10], 71), 0),
        "w_query": noise(key_list[2], (D, QHEADS * HEAD), (1.5 * D ** -0.5), 0.09375, ((0, 16), (1, 2))),
        "w_key": noise(key_list[3], (D, KVHEADS * HEAD), (1.5 * D ** -0.5), 0.09375, ((0, 16),)),
        "w_value": noise(key_list[4], (D, KVHEADS * HEAD), D ** -0.5, 0.0625, ((0, 16),)),
        "bias_query": noise(key_list[5], (QHEADS * HEAD,), 0.5, 3.0, ((0, 2),)),
        "bias_key": noise(key_list[6], (KVHEADS * HEAD,), 0.5, 3.0),
        "bias_value": noise(key_list[7], (KVHEADS * HEAD,), 0.5, 3.0),
        "w_out": noise(key_list[8], (QHEADS * HEAD, D), (QHEADS * HEAD) ** -0.5, 0.09375, ((0, 2), (1, 16))),
        "seq_lengths": uneven(key_list[9], SEQS, TOKENS, LONGEST, 2).astype(jnp.int32),
    }


ROPE_BASE = 1000000.0
EPSILON = 1e-06
FLOOR = -1e+30

def token_layout(seq_lengths, token_index):
    seq_ends = jnp.cumsum(seq_lengths).astype(jnp.int32)
    seq_starts = (seq_ends - seq_lengths).astype(jnp.int32)
    member = (token_index[:, None] >= seq_ends[None, :]).astype(jnp.int32)
    segment = lax.optimization_barrier(jnp.sum(member, axis=1)).astype(jnp.int32)
    one_hot = segment[:, None] == jnp.arange(seq_lengths.shape[0], dtype=jnp.int32)[None, :]
    seq_begin = lax.optimization_barrier(jnp.sum(jnp.where(one_hot, seq_starts[None, :], 0), axis=1)).astype(jnp.int32)
    return (segment, (token_index - seq_begin).astype(jnp.int32))

def rotary(vectors, position):
    half_size = vectors.shape[-1] // 2
    frequency = jnp.exp(jnp.arange(half_size, dtype=jnp.float32) * (-2.0 * math.log(ROPE_BASE) / vectors.shape[-1]))
    angle = position.astype(jnp.float32)[:, None] * frequency[None, :]
    cos_table = jnp.concatenate([jnp.cos(angle), jnp.cos(angle)], axis=1)[:, None, :]
    sin_table = jnp.concatenate([jnp.sin(angle), jnp.sin(angle)], axis=1)[:, None, :]
    turned = jnp.concatenate([-vectors[..., half_size:], vectors[..., :half_size]], axis=-1)
    return vectors * cos_table + turned * sin_table

def rms_normed(hidden, norm_gain):
    widened = hidden.astype(jnp.float32)
    scale = lax.rsqrt(lax.optimization_barrier(jnp.mean(widened * widened, axis=1, keepdims=True)) + EPSILON)
    return (widened * scale * norm_gain.astype(jnp.float32)[None, :]).astype(jnp.bfloat16)

def reference(hidden, norm_gain, w_query, w_key, w_value, bias_query, bias_key, bias_value, w_out, seq_lengths):
    count = hidden.shape[0]
    token_index = jnp.arange(count, dtype=jnp.int32)
    segment, position = token_layout(seq_lengths, token_index)
    normed = rms_normed(hidden, norm_gain)
    query = jnp.dot(normed, w_query, preferred_element_type=jnp.float32) + bias_query.astype(jnp.float32)[None, :]
    keys = jnp.dot(normed, w_key, preferred_element_type=jnp.float32) + bias_key.astype(jnp.float32)[None, :]
    values = jnp.dot(normed, w_value, preferred_element_type=jnp.float32) + bias_value.astype(jnp.float32)[None, :]
    query = rotary(query.reshape(count, QHEADS, HEAD), position).astype(jnp.bfloat16)
    keys = rotary(keys.reshape(count, KVHEADS, HEAD), position).astype(jnp.bfloat16)
    values = values.astype(jnp.bfloat16).reshape(count, KVHEADS, HEAD)
    group = QHEADS // KVHEADS
    block_rows = 256 if count % 256 == 0 else count
    block_count = count // block_rows
    query_blocks = query.reshape(block_count, block_rows, KVHEADS, group, HEAD)
    keys_wide = keys.astype(jnp.float32)
    values_wide = values.astype(jnp.float32)

    def attend_block(query_item):
        query_part, query_segment, query_index = query_item
        scores = jnp.einsum('qkgd,nkd->kgqn', query_part.astype(jnp.float32), keys_wide) * HEAD ** (-0.5)
        allowed = ((query_segment[:, None] == segment[None, :]) & (query_index[:, None] >= token_index[None, :]))[None, None]
        scores = jnp.where(allowed, scores, FLOOR)
        highest = lax.optimization_barrier(jnp.max(scores, axis=3, keepdims=True))
        weights = jnp.where(allowed, jnp.exp(scores - highest), 0.0)
        total = lax.optimization_barrier(jnp.sum(weights, axis=3))
        rounded = weights.astype(jnp.bfloat16).astype(jnp.float32)
        mixed = jnp.einsum('kgqn,nkd->kgqd', rounded, values_wide)
        mixed = mixed / total[..., None]
        return jnp.transpose(mixed, (2, 0, 1, 3)).reshape(block_rows, QHEADS * HEAD)
    attended = lax.map(attend_block, (query_blocks, segment.reshape(block_count, block_rows), token_index.reshape(block_count, block_rows)))
    attended = attended.reshape(count, QHEADS * HEAD).astype(jnp.bfloat16)
    return hidden.astype(jnp.float32) + jnp.dot(attended, w_out, preferred_element_type=jnp.float32)
```

```python
import functools
import math

import jax
import jax.numpy as jnp
from jax import lax
from jax.experimental import pallas as pl
from jax.experimental.pallas import tpu as pltpu
from jax.sharding import PartitionSpec as P

HEAD = 128
QHEADS = 32
KVHEADS = 4

ROPE_BASE = 1000000.0
EPSILON = 1e-06
FLOOR = -1e30
MESH = pl.DeviceIdType.MESH
PARTS = 2


def token_layout(seq_lengths, token_index):
    seq_ends = jnp.cumsum(seq_lengths)
    seq_starts = seq_ends - seq_lengths
    member = (token_index[:, None] >= seq_ends[None, :]).astype(jnp.int32)
    segment = jnp.sum(member, axis=1)
    one_hot = segment[:, None] == jnp.arange(seq_lengths.shape[0], dtype=jnp.int32)[None, :]
    return jnp.sum(jnp.where(one_hot, seq_starts[None, :], 0), axis=1)


def rotary_tables(position):
    half_size = HEAD // 2
    frequency = jnp.exp(
        jnp.arange(half_size, dtype=jnp.float32) * (-2.0 * math.log(ROPE_BASE) / HEAD)
    )
    angle = position.astype(jnp.float32)[:, None] * frequency[None, :]
    cos, sin = jnp.cos(angle), jnp.sin(angle)
    return jnp.concatenate([cos, cos], axis=1), jnp.concatenate([-sin, sin], axis=1)


def gather_kernel(n, block_ref, out_ref, local_sem, send_sem, pass_sem, recv_sem):
    me = lax.axis_index("fsdp")
    partner = me + 1 - 2 * lax.rem(me, 2)
    half = n // 2
    barrier = pltpu.get_barrier_semaphore()
    for d in range(1, half):
        pl.semaphore_signal(
            barrier, inc=1, device_id={"fsdp": lax.rem(me + 2 * d, n)}, device_id_type=MESH
        )
    pl.semaphore_signal(barrier, inc=1, device_id={"fsdp": partner}, device_id_type=MESH)
    pl.semaphore_wait(barrier, half)

    def first(d, target):
        return pltpu.make_async_remote_copy(
            src_ref=block_ref,
            dst_ref=out_ref.at[me],
            send_sem=send_sem.at[d],
            recv_sem=recv_sem.at[me],
            device_id={"fsdp": target},
            device_id_type=MESH,
        )

    def onward(d, source):
        return pltpu.make_async_remote_copy(
            src_ref=out_ref.at[source],
            dst_ref=out_ref.at[source],
            send_sem=pass_sem.at[d],
            recv_sem=recv_sem.at[source],
            device_id={"fsdp": partner},
            device_id_type=MESH,
        )

    own = pltpu.make_async_copy(block_ref, out_ref.at[me], local_sem)
    own.start()
    sends = [first(d, lax.rem(me + 2 * d, n)) for d in range(1, half)] + [first(0, partner)]
    for copy in sends:
        copy.start()
    passes = []
    for d in range(1, half):
        copy = onward(d, lax.rem(me - 2 * d + n, n))
        copy.wait_recv()
        copy.start()
        passes.append(copy)
    onward(0, partner).wait_recv()
    for d in range(1, half):
        onward(d, lax.rem(partner - 2 * d + n, n)).wait_recv()
    for copy in sends + passes:
        copy.wait_send()
    own.wait()


def gather_blocks(block, n):
    rows, cols = block.shape
    if n % 2:
        return lax.all_gather(block, "fsdp", axis=0, tiled=True)
    out = pl.pallas_call(
        functools.partial(gather_kernel, n),
        out_shape=jax.ShapeDtypeStruct((n, rows, cols), block.dtype),
        in_specs=[pl.BlockSpec(memory_space=pltpu.VMEM)],
        out_specs=pl.BlockSpec(memory_space=pltpu.VMEM),
        scratch_shapes=[
            pltpu.SemaphoreType.DMA,
            pltpu.SemaphoreType.DMA((n // 2,)),
            pltpu.SemaphoreType.DMA((n // 2,)),
            pltpu.SemaphoreType.DMA((n,)),
        ],
        compiler_params=pltpu.CompilerParams(collective_id=0, has_side_effects=True),
        cost_estimate=pl.CostEstimate(
            flops=0, bytes_accessed=100_000_000, transcendentals=0
        ),
        name="kv_gather",
    )(block)
    return out.reshape(n * rows, cols)


def attend_kernel(
    block, reach_ref, query_ref, cos_ref, sin_ref, begin_ref, index_ref, key_ref, value_ref, out_ref
):
    query = query_ref[...]
    query = query * cos_ref[...] + pltpu.roll(query, HEAD // 2, 1) * sin_ref[...]
    query = query.astype(jnp.bfloat16)
    rows = query.shape[0]
    begin, index = begin_ref[...], index_ref[...]
    lowest, top = reach_ref[0], reach_ref[1]
    factor = HEAD ** (-0.5) * math.log2(math.e)

    def step(i, carried):
        running, total, summed = carried
        offset = pl.multiple_of((top - i) * block, block)
        scores = lax.dot_general(
            query,
            key_ref[pl.ds(offset, block), :],
            (((1,), (1,)), ((), ())),
            preferred_element_type=jnp.float32,
        )
        place = offset + lax.broadcasted_iota(jnp.int32, (rows, block), 1)
        scores = jnp.where((place >= begin) & (place <= index), scores * factor, FLOOR)
        highest = jnp.maximum(running, jnp.max(scores, axis=1, keepdims=True))
        weights = jnp.exp2(scores - highest)
        shrink = jnp.exp2(running - highest)
        total = total * shrink + jnp.sum(weights, axis=1, keepdims=True)
        update = jnp.dot(
            weights.astype(jnp.bfloat16),
            value_ref[pl.ds(offset, block), :],
            preferred_element_type=jnp.float32,
        )
        return highest, total, summed * shrink + update

    start = (
        jnp.full((rows, 1), FLOOR, jnp.float32),
        jnp.zeros((rows, 1), jnp.float32),
        jnp.zeros((rows, HEAD), jnp.float32),
    )
    running, total, summed = lax.fori_loop(0, top - lowest + 1, step, start)
    out_ref[...] = (summed / total).astype(jnp.bfloat16)


def attend(query, cos, sin, begin, index, pairs, heads, local_kv):
    rows, tokens = query.shape[0], pairs.shape[0]
    block = 2 * rows if tokens % (2 * rows) == 0 else rows
    reach = jnp.stack([begin[0] // block, index[0] // block]).astype(jnp.int32)
    per_kv = heads // local_kv
    whole = lambda width: pl.BlockSpec((rows, width), lambda h: (0, 0))
    return pl.pallas_call(
        functools.partial(attend_kernel, block),
        grid=(heads,),
        out_shape=jax.ShapeDtypeStruct((rows, heads * HEAD), jnp.bfloat16),
        in_specs=[
            pl.BlockSpec(memory_space=pltpu.SMEM),
            pl.BlockSpec((rows, HEAD), lambda h: (0, h)),
            whole(HEAD),
            whole(HEAD),
            whole(1),
            whole(1),
            pl.BlockSpec((tokens, HEAD), lambda h: (0, h // per_kv)),
            pl.BlockSpec((tokens, HEAD), lambda h: (0, local_kv + h // per_kv)),
        ],
        out_specs=pl.BlockSpec((rows, HEAD), lambda h: (0, h)),
        compiler_params=pltpu.CompilerParams(vmem_limit_bytes=24 * 1024 * 1024),
        cost_estimate=pl.CostEstimate(
            flops=4 * rows * tokens * heads * HEAD,
            bytes_accessed=100_000_000,
            transcendentals=rows * tokens * heads,
        ),
        name="attend",
    )(reach, query, cos, sin, begin[:, None], index[:, None], pairs, pairs)


def finish_kernel(parts, others, own_ref, *refs):
    width = own_ref.shape[1] // parts
    out_ref = refs[-1]
    for part in range(parts):
        cut = slice(part * width, (part + 1) * width)
        total = own_ref[:, cut].astype(jnp.float32)
        for term in refs[part * (others + 1) : (part + 1) * (others + 1)]:
            total = total + term[...].astype(jnp.float32)
        out_ref[:, cut] = total


def finish(own_rows, terms, n):
    rows, cols = own_rows.shape
    parts = len(terms)
    wide, narrow = cols // n, cols // n // parts
    return pl.pallas_call(
        functools.partial(finish_kernel, parts, len(terms[0]) - 1),
        grid=(n,),
        out_shape=jax.ShapeDtypeStruct((rows, cols), jnp.float32),
        in_specs=[pl.BlockSpec((rows, wide), lambda f: (0, f))]
        + [pl.BlockSpec((rows, narrow), lambda f: (0, f))] * sum(len(t) for t in terms),
        out_specs=pl.BlockSpec((rows, wide), lambda f: (0, f)),
        compiler_params=pltpu.CompilerParams(vmem_limit_bytes=16 * 1024 * 1024),
        name="finish",
    )(own_rows, *[term for some in terms for term in some])


def shards(
    hidden, norm_gain, w_query, w_key, w_value, bias_query, bias_key, bias_value, w_out, seq_lengths
):
    n, tp = lax.axis_size("fsdp"), lax.axis_size("tp")
    tok_rows = hidden.shape[0]
    query_cols = w_query.shape[1]
    local_heads = query_cols // HEAD
    group_size = QHEADS // KVHEADS
    local_kv = max(local_heads // group_size, 1)
    first_kv = lax.axis_index("tp") * local_heads // group_size
    key_cols = local_kv * HEAD
    key_part = lax.dynamic_slice_in_dim(w_key, first_kv * HEAD, key_cols, 1)
    value_part = lax.dynamic_slice_in_dim(w_value, first_kv * HEAD, key_cols, 1)
    key_bias = lax.dynamic_slice_in_dim(bias_key, first_kv * HEAD, key_cols, 0)
    value_bias = lax.dynamic_slice_in_dim(bias_value, first_kv * HEAD, key_cols, 0)
    weights = lax.all_gather(
        jnp.concatenate([key_part, value_part, w_query], axis=1), "fsdp", axis=0, tiled=True
    )

    local_index = lax.axis_index("fsdp") * tok_rows + jnp.arange(tok_rows, dtype=jnp.int32)
    begin = token_layout(seq_lengths, local_index)
    cos, sin = rotary_tables(local_index - begin)
    widened = hidden.astype(jnp.float32)
    scale = lax.rsqrt(jnp.mean(widened * widened, axis=1, keepdims=True) + EPSILON)
    normed = (widened * scale * norm_gain[None, :]).astype(jnp.bfloat16)

    part_cols = w_out.shape[1] // PARTS
    own_parts = [w_out[:, part * part_cols : (part + 1) * part_cols] for part in range(PARTS)]
    weights, own_parts = lax.optimization_barrier((weights, own_parts))
    out_parts = [lax.all_gather(part, "fsdp", axis=1, tiled=True) for part in own_parts]

    pairs = jnp.dot(normed, weights[:, : 2 * key_cols], preferred_element_type=jnp.float32)
    pairs = pairs + jnp.concatenate([key_bias, value_bias]).astype(jnp.float32)[None, :]
    pieces = []
    for head in range(local_kv):
        one = pairs[:, head * HEAD : (head + 1) * HEAD]
        turned = jnp.concatenate([one[:, HEAD // 2 :], one[:, : HEAD // 2]], axis=1)
        pieces.append(one * cos + turned * sin)
    pieces.append(pairs[:, key_cols:])
    block = jnp.concatenate(pieces, axis=1).astype(jnp.bfloat16)
    query = jnp.dot(normed, weights[:, 2 * key_cols :], preferred_element_type=jnp.float32)
    query = query + bias_query.astype(jnp.float32)[None, :]
    gathered = gather_blocks(block, n)
    attended = attend(query, cos, sin, begin, local_index, gathered, local_heads, local_kv)

    share = tok_rows // tp
    me = lax.axis_index("tp")
    own_rows = lax.dynamic_slice_in_dim(hidden, me * share, share, 0)
    own_attended = lax.dynamic_slice_in_dim(attended, me * share, share, 0)
    terms = []
    for part in range(PARTS):
        some = []
        for d in range(1, tp):
            peer = lax.rem(me + d, tp)
            rows = lax.dynamic_slice_in_dim(attended, peer * share, share, 0)
            term = jnp.dot(rows, out_parts[part], preferred_element_type=jnp.float32)
            some.append(
                lax.ppermute(
                    term.astype(jnp.bfloat16), "tp", [(i, (i + d) % tp) for i in range(tp)]
                )
            )
        some.append(jnp.dot(own_attended, out_parts[part], preferred_element_type=jnp.float32))
        terms.append(some)
    return finish(own_rows, terms, n)


def solution(mesh):
    in_specs = (
        P("fsdp", None),
        P(),
        P("fsdp", "tp"),
        P("fsdp", None),
        P("fsdp", None),
        P("tp"),
        P(),
        P(),
        P("tp", "fsdp"),
        P(),
    )
    out_specs = P(("fsdp", "tp"), None)
    return jax.shard_map(shards, mesh=mesh, in_specs=in_specs, out_specs=out_specs, check_vma=False)
```

```python
import functools
import math

import jax
import jax.numpy as jnp
from jax import lax
from jax.experimental import pallas as pl
from jax.experimental.pallas import tpu as pltpu
from jax.sharding import PartitionSpec as P

HEAD = 128
QHEADS = 32
KVHEADS = 4

ROPE_BASE = 1000000.0
EPSILON = 1e-06
FLOOR = -1e30
MESH = pl.DeviceIdType.MESH
CHUNKS = 4


def token_layout(seq_lengths, token_index):
    seq_ends = jnp.cumsum(seq_lengths)
    seq_starts = seq_ends - seq_lengths
    member = (token_index[:, None] >= seq_ends[None, :]).astype(jnp.int32)
    segment = jnp.sum(member, axis=1)
    one_hot = segment[:, None] == jnp.arange(seq_lengths.shape[0], dtype=jnp.int32)[None, :]
    return jnp.sum(jnp.where(one_hot, seq_starts[None, :], 0), axis=1)


def rotary_tables(position):
    half_size = HEAD // 2
    frequency = jnp.exp(
        jnp.arange(half_size, dtype=jnp.float32) * (-2.0 * math.log(ROPE_BASE) / HEAD)
    )
    angle = position.astype(jnp.float32)[:, None] * frequency[None, :]
    cos, sin = jnp.cos(angle), jnp.sin(angle)
    return jnp.concatenate([cos, cos], axis=1), jnp.concatenate([-sin, sin], axis=1)


def gather_kernel(n, block_ref, out_ref, local_sem, send_sem, recv_sem):
    me = lax.axis_index("fsdp")
    steps = n // 4
    beside = me + 2 - 4 * lax.rem(lax.div(me, 2), 2)
    turn = 1 - 2 * lax.rem(me, 2)
    partner = me + turn
    barrier = pltpu.get_barrier_semaphore()
    for target in [lax.rem(me + 4 * d, n) for d in range(1, steps)] + [beside, partner]:
        pl.semaphore_signal(barrier, inc=1, device_id={"fsdp": target}, device_id_type=MESH)
    pl.semaphore_wait(barrier, steps + 1)

    started = []

    def send(source_ref, source, target):
        copy = pltpu.make_async_remote_copy(
            src_ref=source_ref,
            dst_ref=out_ref.at[source],
            send_sem=send_sem.at[len(started)],
            recv_sem=recv_sem.at[source],
            device_id={"fsdp": target},
            device_id_type=MESH,
        )
        copy.start()
        started.append(copy)

    def arrived(source):
        pltpu.make_async_remote_copy(
            src_ref=block_ref,
            dst_ref=out_ref.at[source],
            send_sem=send_sem.at[0],
            recv_sem=recv_sem.at[source],
            device_id={"fsdp": partner},
            device_id_type=MESH,
        ).wait_recv()

    own = pltpu.make_async_copy(block_ref, out_ref.at[me], local_sem)
    own.start()
    for d in range(1, steps):
        send(block_ref, me, lax.rem(me + 4 * d, n))
    send(block_ref, me, beside)
    send(block_ref, me, partner)
    for d in range(1, steps):
        source = lax.rem(me - 4 * d + n, n)
        arrived(source)
        send(out_ref.at[source], source, beside)
        send(out_ref.at[source], source, partner)
    for d in range(steps):
        source = lax.rem(beside - 4 * d + n, n)
        arrived(source)
        send(out_ref.at[source], source, partner)
    for first in (partner, beside + turn):
        for d in range(steps):
            arrived(lax.rem(first - 4 * d + n, n))
    for copy in started:
        copy.wait_send()
    own.wait()


def gather_blocks(block, n):
    rows, cols = block.shape
    if n % 4:
        return lax.all_gather(block, "fsdp", axis=0, tiled=True)
    out = pl.pallas_call(
        functools.partial(gather_kernel, n),
        out_shape=jax.ShapeDtypeStruct((n, rows, cols), block.dtype),
        in_specs=[pl.BlockSpec(memory_space=pltpu.VMEM)],
        out_specs=pl.BlockSpec(memory_space=pltpu.VMEM),
        scratch_shapes=[
            pltpu.SemaphoreType.DMA,
            pltpu.SemaphoreType.DMA((n,)),
            pltpu.SemaphoreType.DMA((n,)),
        ],
        compiler_params=pltpu.CompilerParams(collective_id=0, has_side_effects=True),
        cost_estimate=pl.CostEstimate(
            flops=0, bytes_accessed=100_000_000, transcendentals=0
        ),
        name="kv_gather",
    )(block)
    return out.reshape(n * rows, cols)


def attend_kernel(
    block, reach_ref, query_ref, cos_ref, sin_ref, begin_ref, index_ref, key_ref, value_ref, out_ref
):
    query = query_ref[...]
    query = query * cos_ref[...] + pltpu.roll(query, HEAD // 2, 1) * sin_ref[...]
    query = query.astype(jnp.bfloat16)
    rows = query.shape[0]
    begin, index = begin_ref[...], index_ref[...]
    lowest, top = reach_ref[0], reach_ref[1]
    factor = HEAD ** (-0.5) * math.log2(math.e)

    def step(i, carried):
        running, total, summed = carried
        offset = pl.multiple_of((top - i) * block, block)
        scores = lax.dot_general(
            query,
            key_ref[pl.ds(offset, block), :],
            (((1,), (1,)), ((), ())),
            preferred_element_type=jnp.float32,
        )
        place = offset + lax.broadcasted_iota(jnp.int32, (rows, block), 1)
        scores = jnp.where((place >= begin) & (place <= index), scores * factor, FLOOR)
        highest = jnp.maximum(running, jnp.max(scores, axis=1, keepdims=True))
        weights = jnp.exp2(scores - highest)
        shrink = jnp.exp2(running - highest)
        total = total * shrink + jnp.sum(weights, axis=1, keepdims=True)
        update = jnp.dot(
            weights.astype(jnp.bfloat16),
            value_ref[pl.ds(offset, block), :],
            preferred_element_type=jnp.float32,
        )
        return highest, total, summed * shrink + update

    start = (
        jnp.full((rows, 1), FLOOR, jnp.float32),
        jnp.zeros((rows, 1), jnp.float32),
        jnp.zeros((rows, HEAD), jnp.float32),
    )
    running, total, summed = lax.fori_loop(0, top - lowest + 1, step, start)
    out_ref[...] = (summed / total).astype(jnp.bfloat16)


def attend(query, cos, sin, begin, index, pairs, heads, local_kv):
    rows, tokens = query.shape[0], pairs.shape[0]
    block = 2 * rows if tokens % (2 * rows) == 0 else rows
    reach = jnp.stack([begin[0] // block, index[0] // block]).astype(jnp.int32)
    per_kv = heads // local_kv
    whole = lambda width: pl.BlockSpec((rows, width), lambda h: (0, 0))
    return pl.pallas_call(
        functools.partial(attend_kernel, block),
        grid=(heads,),
        out_shape=jax.ShapeDtypeStruct((rows, heads * HEAD), jnp.bfloat16),
        in_specs=[
            pl.BlockSpec(memory_space=pltpu.SMEM),
            pl.BlockSpec((rows, HEAD), lambda h: (0, h)),
            whole(HEAD),
            whole(HEAD),
            whole(1),
            whole(1),
            pl.BlockSpec((tokens, HEAD), lambda h: (0, h // per_kv)),
            pl.BlockSpec((tokens, HEAD), lambda h: (0, local_kv + h // per_kv)),
        ],
        out_specs=pl.BlockSpec((rows, HEAD), lambda h: (0, h)),
        compiler_params=pltpu.CompilerParams(vmem_limit_bytes=24 * 1024 * 1024),
        cost_estimate=pl.CostEstimate(
            flops=4 * rows * tokens * heads * HEAD,
            bytes_accessed=100_000_000,
            transcendentals=rows * tokens * heads,
        ),
        name="attend",
    )(reach, query, cos, sin, begin[:, None], index[:, None], pairs, pairs)


def finish_kernel(base_ref, *refs):
    out_ref = refs[-1]
    width = refs[0].shape[1]
    chunks = base_ref.shape[1] // width
    for chunk in range(chunks):
        cut = slice(chunk * width, (chunk + 1) * width)
        total = base_ref[:, cut]
        for term in refs[chunk:-1:chunks]:
            total = total + term[...].astype(jnp.float32)
        out_ref[:, cut] = total


def finish(base, received):
    rows, cols = base.shape
    some = rows // 4 if rows % 64 == 0 else rows
    return pl.pallas_call(
        finish_kernel,
        grid=(rows // some,),
        out_shape=jax.ShapeDtypeStruct((rows, cols), jnp.float32),
        in_specs=[pl.BlockSpec((some, cols), lambda r: (r, 0))]
        + [pl.BlockSpec((some, cols // CHUNKS), lambda r: (r, 0))] * len(received),
        out_specs=pl.BlockSpec((some, cols), lambda r: (r, 0)),
        compiler_params=pltpu.CompilerParams(vmem_limit_bytes=16 * 1024 * 1024),
        name="finish",
    )(base, *received)


def shards(
    hidden, norm_gain, w_query, w_key, w_value, bias_query, bias_key, bias_value, w_out, seq_lengths
):
    n, tp = lax.axis_size("fsdp"), lax.axis_size("tp")
    tok_rows = hidden.shape[0]
    query_cols = w_query.shape[1]
    local_heads = query_cols // HEAD
    group_size = QHEADS // KVHEADS
    local_kv = max(local_heads // group_size, 1)
    first_kv = lax.axis_index("tp") * local_heads // group_size
    key_cols = local_kv * HEAD
    key_part = lax.dynamic_slice_in_dim(w_key, first_kv * HEAD, key_cols, 1)
    value_part = lax.dynamic_slice_in_dim(w_value, first_kv * HEAD, key_cols, 1)
    key_bias = lax.dynamic_slice_in_dim(bias_key, first_kv * HEAD, key_cols, 0)
    value_bias = lax.dynamic_slice_in_dim(bias_value, first_kv * HEAD, key_cols, 0)
    weights = lax.all_gather(
        jnp.concatenate([key_part, value_part, w_query], axis=1), "fsdp", axis=0, tiled=True
    )

    local_index = lax.axis_index("fsdp") * tok_rows + jnp.arange(tok_rows, dtype=jnp.int32)
    begin = token_layout(seq_lengths, local_index)
    cos, sin = rotary_tables(local_index - begin)
    widened = hidden.astype(jnp.float32)
    scale = lax.rsqrt(jnp.mean(widened * widened, axis=1, keepdims=True) + EPSILON)
    normed = (widened * scale * norm_gain[None, :]).astype(jnp.bfloat16)

    weights, w_out = lax.optimization_barrier((weights, w_out))
    w_out = lax.all_gather(w_out, "fsdp", axis=1, tiled=True)

    pairs = jnp.dot(normed, weights[:, : 2 * key_cols], preferred_element_type=jnp.float32)
    pairs = pairs + jnp.concatenate([key_bias, value_bias]).astype(jnp.float32)[None, :]
    pieces = []
    for head in range(local_kv):
        one = pairs[:, head * HEAD : (head + 1) * HEAD]
        turned = jnp.concatenate([one[:, HEAD // 2 :], one[:, : HEAD // 2]], axis=1)
        pieces.append(one * cos + turned * sin)
    pieces.append(pairs[:, key_cols:])
    block = jnp.concatenate(pieces, axis=1).astype(jnp.bfloat16)
    query = jnp.dot(normed, weights[:, 2 * key_cols :], preferred_element_type=jnp.float32)
    query = query + bias_query.astype(jnp.float32)[None, :]
    gathered = gather_blocks(block, n)
    attended = attend(query, cos, sin, begin, local_index, gathered, local_heads, local_kv)

    share = tok_rows // tp
    me = lax.axis_index("tp")
    own_rows = lax.dynamic_slice_in_dim(hidden, me * share, share, 0)
    own_attended = lax.dynamic_slice_in_dim(attended, me * share, share, 0)
    width = w_out.shape[1] // CHUNKS
    received = []
    for d in range(1, tp):
        rows = lax.dynamic_slice_in_dim(attended, lax.rem(me + d, tp) * share, share, 0)
        for chunk in range(CHUNKS):
            term = jnp.dot(
                rows,
                w_out[:, chunk * width : (chunk + 1) * width],
                preferred_element_type=jnp.float32,
            )
            received.append(
                lax.ppermute(
                    term.astype(jnp.bfloat16), "tp", [(i, (i + d) % tp) for i in range(tp)]
                )
            )
    base = jnp.dot(own_attended, w_out, preferred_element_type=jnp.float32)
    return finish(base + own_rows.astype(jnp.float32), received)


def solution(mesh):
    in_specs = (
        P("fsdp", None),
        P(),
        P("fsdp", "tp"),
        P("fsdp", None),
        P("fsdp", None),
        P("tp"),
        P(),
        P(),
        P("tp", "fsdp"),
        P(),
    )
    out_specs = P(("fsdp", "tp"), None)
    return jax.shard_map(shards, mesh=mesh, in_specs=in_specs, out_specs=out_specs, check_vma=False)
```
